32 devices in a mesh: gx: 4 (over y, x), gy: 8 (over z, core).
Axes of the slice: x: 2, y: 2, z: 4, core: 2. Of those that a mesh axis runs over, the one named last changes fastest.
Arguments:
- tile_flux: bfloat16 [4, 12, 8, 131072], P(None, None, None, ('gx', 'gy')), may hold values from -6 to 6
- tile_frac: float32 [8, 131072], P(None, ('gx', 'gy')), may hold values from 0.02 to 1
- weights: bfloat16 [32, 7, 16, 256, 128], P(('gx', 'gy')), may hold values from -0.049804688 to 0.14941406
- block_row: int32 [32, 7, 16], P(('gx', 'gy')), may hold values from 0 to 47
- block_col: int32 [32, 7, 16], P(('gx', 'gy')), may hold values from 0 to 31
- send_counts: int32 [32, 7], P(('gx', 'gy')), may hold values from 1 to 16, as said below
Outputs:
- atm_flux: float32 [4, 12, 393216], P(None, None, ('gx', 'gy'))
The draws below stay inside these ranges and needn't reach their ends.
Inputs may be any that keep to these rules, and one draw needn't show every extreme that they name: `send_counts`: live slots of a device at an offset; some device has all 7 offsets at 16, and some device receives 16 live slots from every offset.
All inputs are finite; a program needn't handle non-finite values.
Results may differ from the reference program's by a relative error of at most 0.0029.
Values sent between devices are 32-bit elements; how exact they have to be, the bound alone decides.
No kernel may reach another device: no remote copies, remote signals or barrier semaphores. Data moves between devices by JAX's collectives and lax.ppermute only.
A program may use at most 128 MiB of HBM per device.

```python
import math
import jax
import jax.numpy as jnp
from jax import lax

NFLUX = 12
TILES = 8
SUBSTEPS = 4
BROWS = 256
LCOLS = 128
REACH = 3
CAP = 16
LB_DEV = 32
AB_DEV = 48
NOFF = 7
LAND_CELLS = 131072
ATM_CELLS = 393216
DEVICES = 32


def draw_send_counts(key, part):
    key_base, key_full = jax.random.split(jax.random.fold_in(key, 17))
    base = jax.random.randint(key_base, (DEVICES, NOFF), 1, CAP // 2 + 1)
    full_dev = jax.random.randint(key_full, (), 0, DEVICES)
    row_ids = jnp.arange(DEVICES, dtype=jnp.int32)[:, None]
    col_ids = jnp.arange(NOFF, dtype=jnp.int32)[None, :]
    source = (full_dev - (col_ids - REACH)) % DEVICES
    filled = (row_ids == full_dev) | (row_ids == source)
    return jnp.where(filled, CAP, base).astype(jnp.int32)


def plant(values, key, least, top_value):
    spot = [jax.random.randint(jax.random.fold_in(key, axis), (), 0, length) for axis, length in enumerate(values.shape)]
    widest = values.shape.index(max(values.shape))
    next_to = spot[:widest] + [(spot[widest] + 1) % values.shape[widest]] + spot[widest + 1:]
    return values.at[tuple(spot)].set(least).at[tuple(next_to)].set(top_value)


def block_scale(own_key, extent, cuts, low, high):
    factor_of = 1.0
    for axis_at, shards_of in cuts:
        steps = jax.random.uniform(jax.random.fold_in(jax.random.fold_in(own_key, 6), axis_at), (shards_of,), jnp.float32, low / len(cuts), high / len(cuts))
        factor_of = factor_of * jnp.repeat(jnp.exp(steps), extent[axis_at] // shards_of).reshape((-1,) + (1,) * (len(extent) - 1 - axis_at))
    return factor_of


def bell_draw(stream_key, extent, spread, bound, cuts=(), held_as=jnp.bfloat16):
    result = spread * jax.random.normal(stream_key, extent, jnp.float32)
    if cuts:
        result = result * block_scale(stream_key, extent, cuts, -0.22, 0.18)
    return jnp.clip(result, -bound, bound).astype(held_as)


def setup_inputs(seed: int = 0) -> dict:
    streams_of = jax.random.split(jax.random.key(seed), 7)
    tile_flux = bell_draw(streams_of[0], (SUBSTEPS, NFLUX, TILES, LAND_CELLS), 1.0, 6.0, ((3, 32),))
    tile_frac = jnp.clip(jnp.exp(math.log(1.0) - 3.912023 * jax.random.uniform(streams_of[1], (TILES, LAND_CELLS), jnp.float32) ** block_scale(streams_of[1], (TILES, LAND_CELLS), ((1, 32),), -0.2, 0.2)), 0.02, 1.0)
    weights = jnp.clip(-0.049804688 + 0.19921875 * jax.random.uniform(streams_of[2], (DEVICES, NOFF, CAP, BROWS, LCOLS), jnp.float32) ** block_scale(streams_of[2], (DEVICES, NOFF, CAP, BROWS, LCOLS), ((0, 32),), -0.2, 0.2), -0.049804688, 0.14941406).astype(jnp.bfloat16)
    block_row = plant(jax.random.randint(streams_of[3], (DEVICES, NOFF, CAP), 0, AB_DEV), jax.random.fold_in(streams_of[3], 1), 0, AB_DEV - 1).astype(jnp.int32)
    block_col = plant(jax.random.randint(streams_of[4], (DEVICES, NOFF, CAP), 0, LB_DEV), jax.random.fold_in(streams_of[4], 1), 0, LB_DEV - 1).astype(jnp.int32)
    send_counts = draw_send_counts(jax.random.fold_in(streams_of[6], 71), 0)
    return {"tile_flux": tile_flux, "tile_frac": tile_frac, "weights": weights, "block_row": block_row, "block_col": block_col, "send_counts": send_counts}


def reference(tile_flux, tile_frac, weights, block_row, block_col, send_counts):
    frac_sum = jnp.sum(tile_frac, axis=0)
    merged = (jnp.sum(tile_flux.astype(jnp.float32) * tile_frac[None, None], axis=2) / frac_sum).astype(jnp.bfloat16)
    width = SUBSTEPS * NFLUX
    land_blocks = merged.reshape(width, DEVICES, LB_DEV, LCOLS).transpose(1, 2, 0, 3)

    def one_device(block_w, columns, counts, blocks):
        picked = blocks[columns]
        partial_value = jnp.einsum('okrc,okfc->okfr', block_w.astype(jnp.float32), picked.astype(jnp.float32))
        active = (jnp.arange(CAP, dtype=jnp.int32)[None, :] < counts[:, None]).astype(jnp.float32)
        return partial_value * active[:, :, None, None]

    def one_group(items):
        return jax.vmap(one_device)(*items)

    group = 8
    grouped = (weights.reshape((DEVICES // group, group) + weights.shape[1:]),
               block_col.reshape((DEVICES // group, group) + block_col.shape[1:]),
               send_counts.reshape((DEVICES // group, group) + send_counts.shape[1:]),
               land_blocks.reshape((DEVICES // group, group) + land_blocks.shape[1:]))
    partials = lax.map(one_group, grouped)
    dest_dev = (jnp.arange(DEVICES, dtype=jnp.int32)[:, None] + jnp.arange(NOFF, dtype=jnp.int32)[None, :] - REACH) % DEVICES
    target = (dest_dev[:, :, None] * AB_DEV + block_row).astype(jnp.int32)
    totals = jnp.zeros((DEVICES * AB_DEV, width, BROWS), jnp.float32)
    totals = totals.at[target.reshape(-1)].add(partials.reshape(-1, width, BROWS))
    return totals.transpose(1, 0, 2).reshape(SUBSTEPS, NFLUX, ATM_CELLS)
```

```python
import functools

import jax
import jax.numpy as jnp
from jax import lax
from jax.experimental import pallas as pl
from jax.experimental.pallas import tpu as pltpu
from jax.sharding import PartitionSpec as P

AXES = ("gx", "gy")
AB_DEV = 48
LANES = 128
SUBLANES = 8


def fold_rows(parts):
    row = lax.broadcasted_iota(jnp.int32, parts[0].shape, 0)
    step = SUBLANES // 2
    while step >= 1:
        low = (row // step) % 2 == 0
        half = len(parts) // 2
        merged = []
        for index in range(half):
            first, second = parts[index], parts[index + half]
            keep = jnp.where(low, first, second)
            swap = jnp.where(low, second, first)
            merged.append(keep + jnp.where(low, pltpu.roll(first, SUBLANES - step, 0), pltpu.roll(second, step, 0)))
            del swap
        parts = merged
        step //= 2
    return parts[0]


def merge_kernel(flux_ref, frac_ref, out_ref):
    steps, kinds = flux_ref.shape[0], flux_ref.shape[1]
    rows = steps * kinds

    def one_block(index, carry):
        lanes = pl.ds(pl.multiple_of(index * LANES, LANES), LANES)
        frac = frac_ref[:, lanes]
        total = jnp.sum(frac, axis=0, keepdims=True)
        for pair in range(rows // (2 * SUBLANES)):
            pieces = []
            for half in range(2):
                parts = []
                for r in range(SUBLANES):
                    line = (2 * pair + half) * SUBLANES + r
                    parts.append(flux_ref[line % steps, line // steps, :, lanes].astype(jnp.float32) * frac)
                pieces.append(fold_rows(parts) / total)
            value = jnp.concatenate(pieces, axis=0).astype(jnp.bfloat16)
            out_ref[index, pl.ds(pair * 2 * SUBLANES, 2 * SUBLANES), :] = value
        return carry

    lax.fori_loop(0, out_ref.shape[0], one_block, 0)


def merge(tile_flux, tile_frac, block_cols):
    steps, kinds, tiles, cells = tile_flux.shape
    blocks = cells // block_cols
    group = max(g for g in range(1, 9) if blocks % g == 0)
    return pl.pallas_call(
        merge_kernel,
        grid=(blocks // group,),
        in_specs=[
            pl.BlockSpec((steps, kinds, tiles, group * block_cols), lambda i: (0, 0, 0, i)),
            pl.BlockSpec((tiles, group * block_cols), lambda i: (0, i)),
        ],
        out_specs=pl.BlockSpec((group, steps * kinds, block_cols), lambda i: (i, 0, 0)),
        out_shape=jax.ShapeDtypeStruct((blocks, steps * kinds, block_cols), jnp.bfloat16),
        name="merge",
    )(tile_flux, tile_frac)


def product_kernel(cols_ref, counts_ref, land_ref, *refs, chunks):
    for index, (offset, first) in enumerate(chunks):
        w_ref = refs[index]
        out_ref = refs[len(chunks) + index]
        for slot in range(out_ref.shape[0]):

            @pl.when(first + slot < counts_ref[0, offset])
            def _():
                out_ref[slot] = lax.dot_general(
                    land_ref[cols_ref[0, offset, first + slot]],
                    w_ref[0, 0, slot],
                    (((1,), (1,)), ((), ())),
                    preferred_element_type=jnp.float32,
                )


def products(block_col, counts, land, weights, chunks, width):
    _, _, _, rows, cols = weights.shape
    blocks, nf, _ = land.shape
    return pl.pallas_call(
        functools.partial(product_kernel, chunks=chunks),
        grid=(1,),
        in_specs=[
            pl.BlockSpec(memory_space=pltpu.SMEM),
            pl.BlockSpec(memory_space=pltpu.SMEM),
            pl.BlockSpec((blocks, nf, cols), lambda i: (0, 0, 0)),
        ]
        + [
            pl.BlockSpec((1, 1, width, rows, cols), lambda i, o=o, f=f: (0, o, f // width, 0, 0))
            for o, f in chunks
        ],
        out_specs=[pl.BlockSpec((width, nf, rows), lambda i: (0, 0, 0)) for _ in chunks],
        out_shape=[jax.ShapeDtypeStruct((width, nf, rows), jnp.float32) for _ in chunks],
        name="products",
    )(block_col, counts, land, *([weights] * len(chunks)))


def settle_kernel(meta_ref, *refs, first, fresh):
    arrivals = refs[: len(first)]
    totals = refs[len(first) if fresh else len(first) + 1]
    if fresh:
        totals[...] = jnp.zeros(totals.shape, totals.dtype)
    else:
        totals[...] = refs[len(first)][...]
    kinds = totals.shape[0]
    steps = totals.shape[2] // 2
    row = lax.broadcasted_iota(jnp.int32, (2 * steps, LANES), 0)
    low = row < steps
    for index, arrival in enumerate(arrivals):
        base = first[index]
        live = jnp.clip(meta_ref[index, 0] - base, 0, arrival.shape[0])

        def one_slot(slot, carry, index=index, arrival=arrival, base=base):
            block = meta_ref[index, 1 + base + slot]
            for pair in range(kinds // 2):
                lines = pl.ds(pair * 2 * steps, 2 * steps)
                left = arrival[slot, lines, pl.ds(0, LANES)]
                right = arrival[slot, lines, pl.ds(LANES, LANES)]
                even = jnp.where(low, left, pltpu.roll(right, steps, 0))
                odd = jnp.where(low, pltpu.roll(left, steps, 0), right)
                totals[2 * pair, block] += even
                totals[2 * pair + 1, block] += odd
            return carry

        lax.fori_loop(0, live, one_slot, 0)


def settle(meta, arrivals, first, shape, totals=None):
    fresh = totals is None
    given = list(arrivals) + ([] if fresh else [totals])
    return pl.pallas_call(
        functools.partial(settle_kernel, first=first, fresh=fresh),
        in_specs=[pl.BlockSpec(memory_space=pltpu.SMEM)]
        + [pl.BlockSpec(memory_space=pltpu.VMEM) for _ in given],
        out_specs=pl.BlockSpec(memory_space=pltpu.VMEM),
        out_shape=jax.ShapeDtypeStruct(shape, jnp.float32),
        input_output_aliases={} if fresh else {len(given): 0},
        name="settle",
    )(meta, *given)


def spread(info, count):
    held = info[None]
    span = 1
    exact = count & (count - 1) == 0
    while span < count:
        if exact:
            pairs = [(d, d ^ span) for d in range(count)]
        else:
            pairs = [(d, (d + span) % count) for d in range(count)]
        held = jnp.concatenate([held, lax.ppermute(held, AXES, pairs)], axis=0)
        span *= 2
    return held, exact


def on_device(tile_flux, tile_frac, weights, block_row, block_col, send_counts):
    steps, kinds = tile_flux.shape[0], tile_flux.shape[1]
    _, num_off, slots, block_rows, block_cols = weights.shape
    count = lax.axis_size(AXES)
    here = lax.axis_index(AXES)
    reach = num_off // 2
    width = slots // 2
    shifts = [o - reach for o in range(num_off)]
    away = sorted((o for o in range(num_off) if o != reach), key=lambda o: -abs(shifts[o]))
    modulus = min(m for m in range(num_off, count + num_off) if count % m == 0 or m >= count)
    shape = (kinds, AB_DEV, 2 * steps, block_rows // 2)

    own = jnp.concatenate([send_counts[0][:, None], block_row[0]], axis=1)
    held, exact = spread(own, count)
    index = jnp.arange(held.shape[0], dtype=jnp.int32)
    source = (here ^ index) if exact else (here - index) % count
    target = (source[:, None] + jnp.array(shifts, jnp.int32)[None, :]) % count
    over = (held[:, :, 0] > width) & (jnp.array(shifts, jnp.int32) != 0)[None, :]
    kind = jnp.arange(modulus, dtype=jnp.int32)
    loose = over[:, :, None] & (source[:, None, None] % modulus != kind) & (target[:, :, None] % modulus != kind)
    loose = jnp.any(loose, axis=(0, 1))
    plan = jnp.min(jnp.where(loose, modulus, kind))
    senders = [(here - shifts[o]) % count for o in range(num_off)]
    places = jnp.stack([(here ^ s) if exact else (here - s) % count for s in senders])
    meta = held[places, jnp.arange(num_off)]

    land = merge(tile_flux, tile_frac, block_cols)
    base = {}
    for a, b in ((away[0], away[1]), (away[2], away[3]), (away[4], away[5])):
        base[a], base[b] = products(block_col, send_counts, land, weights, ((a, 0), (b, 0)), width)
    more = products(block_col, send_counts, land, weights, tuple((o, width) for o in away), width)
    mine = products(block_col, send_counts, land, weights, ((reach, 0), (reach, width)), width)

    def everyone(o):
        return [(s, (s + shifts[o]) % count) for s in range(count)]

    def around(o, which):
        return [(s, t) for s, t in everyone(o) if s % modulus == which or t % modulus == which]

    arrived = [lax.ppermute(base[o], AXES, everyone(o)) for o in away]

    def branch(which):
        def send(*values):
            return tuple(
                lax.ppermute(v, AXES, everyone(o) if which == modulus else around(o, which))
                for o, v in zip(away, values)
            )

        return send

    extra = lax.switch(plan, [branch(w) for w in range(modulus + 1)], *more)
    totals = settle(meta[reach][None], mine[:1], (0,), shape)
    metas = jnp.concatenate([meta[reach][None], meta[jnp.array(away)]])
    totals = settle(metas, (mine[1], *arrived), (width,) + (0,) * len(away), shape, totals)
    totals = settle(meta[jnp.array(away)], extra, (width,) * len(away), shape, totals)
    totals = totals.reshape(kinds, AB_DEV, 2, steps, block_rows // 2).transpose(3, 0, 1, 2, 4)
    return totals.reshape(steps, kinds, AB_DEV * block_rows)


def solution(mesh):
    return jax.shard_map(
        on_device,
        mesh=mesh,
        in_specs=(
            P(None, None, None, AXES),
            P(None, AXES),
            P(AXES, None, None, None, None),
            P(AXES, None, None),
            P(AXES, None, None),
            P(AXES, None),
        ),
        out_specs=P(None, None, AXES),
        check_vma=False,
    )
```

```python
import functools
import itertools

import jax
import jax.numpy as jnp
from jax import lax
from jax.experimental import pallas as pl
from jax.experimental.pallas import tpu as pltpu
from jax.sharding import PartitionSpec as P


AXES = ("gx", "gy")
AB_DEV = 48
LANES = 128
SUBLANES = 8


def fold_rows(parts):
    row = lax.broadcasted_iota(jnp.int32, parts[0].shape, 0)
    step = SUBLANES // 2
    while step >= 1:
        low = (row // step) % 2 == 0
        half = len(parts) // 2
        merged = []
        for index in range(half):
            first, second = parts[index], parts[index + half]
            keep = jnp.where(low, first, second)
            swap = jnp.where(low, second, first)
            merged.append(keep + jnp.where(low, pltpu.roll(first, SUBLANES - step, 0), pltpu.roll(second, step, 0)))
            del swap
        parts = merged
        step //= 2
    return parts[0]


def merge_blocks(flux_ref, frac_ref, land_ref, first, count):
    steps, kinds = flux_ref.shape[0], flux_ref.shape[1]
    rows = steps * kinds

    @pl.loop(0, count, unroll=2)
    def _(index):
        lanes = pl.ds(pl.multiple_of(index * LANES, LANES), LANES)
        frac = frac_ref[:, pl.ds(pl.multiple_of((first + index) * LANES, LANES), LANES)]
        total = jnp.sum(frac, axis=0, keepdims=True)
        for pair in range(rows // (2 * SUBLANES)):
            pieces = []
            for half in range(2):
                parts = []
                for r in range(SUBLANES):
                    line = (2 * pair + half) * SUBLANES + r
                    parts.append(flux_ref[line % steps, line // steps, :, lanes].astype(jnp.float32) * frac)
                pieces.append(fold_rows(parts) / total)
            value = jnp.concatenate(pieces, axis=0).astype(jnp.bfloat16)
            land_ref[first + index, pl.ds(pair * 2 * SUBLANES, 2 * SUBLANES), :] = value


def block_product(land_ref, col, w_ref, local):
    return lax.dot_general(
        land_ref[col], w_ref[0, 0, local], (((1,), (1,)), ((), ())), preferred_element_type=jnp.float32
    )


def first_kernel(offs_ref, cols_ref, counts_ref, flux, frac, weights, land_out, *refs, entries, ranks):
    far = len(entries)
    outs, refs = refs[: far + ranks], refs[far + ranks :]
    flux_v, frac_v, w_v, land_v, near_v, piece_v, in_sems, w_sems, out_sems = refs
    groups, half = flux_v.shape[0], w_v.shape[1]
    wide = flux_v.shape[-1]
    piece = piece_v.shape[2]
    blocks = land_v.shape[0] // groups

    def load_flux(i):
        return pltpu.make_async_copy(flux.at[:, :, :, pl.ds(i * wide, wide)], flux_v.at[i], in_sems.at[1 + i])

    def load_weights(index, part):
        source = weights.at[0, offs_ref[entries[index]], pl.ds(part * half, half)]
        return pltpu.make_async_copy(source, w_v.at[part * far + index], w_sems.at[part * far + index])

    def crowded(index):
        return counts_ref[0, offs_ref[entries[index]]] > half

    load_frac = pltpu.make_async_copy(frac, frac_v, in_sems.at[0])
    load_frac.start()
    for i in range(groups):
        load_flux(i).start()
    for index in range(far):
        load_weights(index, 0).start()
    for index in range(far):

        @pl.when(crowded(index))
        def _():
            load_weights(index, 1).start()

    load_frac.wait()
    for i in range(groups):
        load_flux(i).wait()
        merge_blocks(flux_v.at[i], frac_v, land_v, i * blocks, blocks)
    stores = [pltpu.make_async_copy(land_v, land_out, out_sems.at[far + ranks])]
    stores[0].start()
    for index, entry in enumerate(entries):
        load_weights(index, 0).wait()
        for local in range(half):
            near_v[index, local] = lax.dot_general(
                land_v[cols_ref[offs_ref[entry], 0, local]],
                w_v[index, local],
                (((1,), (1,)), ((), ())),
                preferred_element_type=jnp.float32,
            )
        stores.append(pltpu.make_async_copy(near_v.at[index], outs[index], out_sems.at[index]))
        stores[-1].start()
    for index, entry in enumerate(entries):

        @pl.when(crowded(index))
        def _():
            load_weights(index, 1).wait()
            for local in range(half):
                piece_v[local // piece, index, local % piece] = lax.dot_general(
                    land_v[cols_ref[offs_ref[entry], 0, half + local]],
                    w_v[far + index, local],
                    (((1,), (1,)), ((), ())),
                    preferred_element_type=jnp.float32,
                )

    for k in range(ranks):
        stores.append(pltpu.make_async_copy(piece_v.at[k], outs[far + k], out_sems.at[far + k]))
        stores[-1].start()
    for store in stores:
        store.wait()


def first_products(tables, tile_flux, tile_frac, weights, entries, ranks, piece):
    steps, kinds, tiles, cells = tile_flux.shape
    _, _, slots, rows, cols = weights.shape
    nf, blocks, half, far = steps * kinds, cells // cols, slots // 2, len(entries)
    groups = min(g for g in range(1, blocks + 1) if blocks % g == 0 and blocks // g <= 4)
    anywhere = pl.BlockSpec(memory_space=pl.ANY)
    return pl.pallas_call(
        functools.partial(first_kernel, entries=entries, ranks=ranks),
        in_specs=[pl.BlockSpec(memory_space=pltpu.SMEM)] * 3 + [anywhere] * 3,
        out_specs=[anywhere] * (1 + far + ranks),
        out_shape=[jax.ShapeDtypeStruct((blocks, nf, cols), jnp.bfloat16)]
        + [jax.ShapeDtypeStruct((half, nf, rows), jnp.float32) for _ in entries]
        + [jax.ShapeDtypeStruct((far, piece, nf, rows), jnp.float32) for _ in range(ranks)],
        scratch_shapes=[
            pltpu.VMEM((groups, steps, kinds, tiles, cells // groups), tile_flux.dtype),
            pltpu.VMEM(tile_frac.shape, tile_frac.dtype),
            pltpu.VMEM((2 * far, half, rows, cols), weights.dtype),
            pltpu.VMEM((blocks, nf, cols), jnp.bfloat16),
            pltpu.VMEM((far, half, nf, rows), jnp.float32),
            pltpu.VMEM((ranks, far, piece, nf, rows), jnp.float32),
            pltpu.SemaphoreType.DMA((1 + groups,)),
            pltpu.SemaphoreType.DMA((2 * far,)),
            pltpu.SemaphoreType.DMA((far + ranks + 1,)),
        ],
        name="first",
    )(*tables, tile_flux, tile_frac, weights)


def product_kernel(offs_ref, cols_ref, counts_ref, land_ref, *refs, chunks):
    for index, (entry, first) in enumerate(chunks):
        w_ref = refs[index]
        out_ref = refs[len(chunks) + index]
        offset = offs_ref[entry]
        for start in range(0, out_ref.shape[0], SUBLANES):

            @pl.when(first + start < counts_ref[0, offset])
            def _():
                for local in range(start, min(start + SUBLANES, out_ref.shape[0])):
                    out_ref[local] = block_product(land_ref, cols_ref[offset, 0, first + local], w_ref, local)


def products(tables, land, weights, chunks, width):
    _, _, _, rows, cols = weights.shape
    blocks, nf, _ = land.shape
    return pl.pallas_call(
        functools.partial(product_kernel, chunks=chunks),
        grid_spec=pltpu.PrefetchScalarGridSpec(
            num_scalar_prefetch=3,
            grid=(1,),
            in_specs=[pl.BlockSpec((blocks, nf, cols), lambda i, *_: (0, 0, 0))]
            + [
                pl.BlockSpec((1, 1, width, rows, cols), lambda i, offs, *_, e=e, f=f: (0, offs[e], f // width, 0, 0))
                for e, f in chunks
            ],
            out_specs=[pl.BlockSpec((width, nf, rows), lambda i, *_: (0, 0, 0)) for _ in chunks],
        ),
        out_shape=[jax.ShapeDtypeStruct((width, nf, rows), jnp.float32) for _ in chunks],
        name="products",
    )(*tables, land, *([weights] * len(chunks)))


def choose_kernel(offs_ref, counts_ref, *refs, entries, half):
    ranks = len(refs) - 1 - len(entries)
    outs, sems = refs[ranks:-1], refs[-1]
    for go in (True, False):
        for index, entry in enumerate(entries):
            pick = jnp.int32(0)
            for rank in reversed(range(ranks)):
                pick = jnp.where(counts_ref[rank, offs_ref[entry]] > half, rank, pick)
            for rank in range(ranks):

                @pl.when(pick == rank)
                def _():
                    copy = pltpu.make_async_copy(refs[rank].at[index], outs[index], sems.at[index])
                    copy.start() if go else copy.wait()


def choose(offs, counts, givens, entries, half):
    return pl.pallas_call(
        functools.partial(choose_kernel, entries=entries, half=half),
        in_specs=[pl.BlockSpec(memory_space=pltpu.SMEM)] * 2 + [pl.BlockSpec(memory_space=pl.ANY)] * len(givens),
        out_specs=[pl.BlockSpec(memory_space=pltpu.VMEM)] * len(entries),
        out_shape=[jax.ShapeDtypeStruct(givens[0].shape[1:], jnp.float32)] * len(entries),
        scratch_shapes=[pltpu.SemaphoreType.DMA((len(entries),))],
        name="choose",
    )(offs, counts, *givens)


def pack_kernel(*refs):
    givens, out, sems = refs[:-2], refs[-2], refs[-1]
    copies = [pltpu.make_async_copy(g, out.at[i], sems.at[i]) for i, g in enumerate(givens)]
    for copy in copies:
        copy.start()
    for copy in copies:
        copy.wait()


def pack(givens):
    return pl.pallas_call(
        pack_kernel,
        in_specs=[pl.BlockSpec(memory_space=pl.ANY)] * len(givens),
        out_specs=pl.BlockSpec(memory_space=pltpu.VMEM),
        out_shape=jax.ShapeDtypeStruct((len(givens), *givens[0].shape), jnp.float32),
        scratch_shapes=[pltpu.SemaphoreType.DMA((len(givens),))],
        name="pack",
    )(*givens)


def settle_kernel(rows_ref, *refs, entries, count, fresh):
    rest = refs[count:]
    given = None if fresh else rest[0]
    out, totals, held, sems, moves = rest[-5:]
    last = rows_ref.shape[0] - 1

    def live(entry):
        _, _, row, first, limit, _, fast = entries[entry]
        number = jnp.clip(rows_ref[row, 0] - first, 0, limit)
        return jnp.where(rows_ref[last, 0] > 0, 0, number) if fast else number

    def copy(entry, slot):
        index, sub, place = entries[entry][0], entries[entry][1], entries[entry][5]
        source = refs[index].at[slot] if sub is None else refs[index].at[sub, slot]
        return pltpu.make_async_copy(source, held.at[place + slot], sems.at[place + slot])

    for entry in range(len(entries)):

        @pl.loop(0, live(entry))
        def _(slot, entry=entry):
            copy(entry, slot).start()

    if fresh:
        totals[...] = jnp.zeros(totals.shape, totals.dtype)
    else:
        load = pltpu.make_async_copy(given, totals, moves.at[0])
        load.start()
        load.wait()
    kinds = totals.shape[0]
    steps = totals.shape[2] // 2
    low = lax.broadcasted_iota(jnp.int32, (2 * steps, LANES), 0) < steps
    for entry in range(len(entries)):

        @pl.loop(0, live(entry))
        def _(slot, entry=entry):
            copy(entry, slot).wait()
            _, _, row, first, _, start, _ = entries[entry]
            block = rows_ref[row, 1 + first + slot]
            for pair in range(kinds // 2):
                lines = pl.ds(pair * 2 * steps, 2 * steps)
                left = held[start + slot, lines, pl.ds(0, LANES)]
                right = held[start + slot, lines, pl.ds(LANES, LANES)]
                totals[2 * pair, block] += jnp.where(low, left, pltpu.roll(right, steps, 0))
                totals[2 * pair + 1, block] += jnp.where(low, pltpu.roll(left, steps, 0), right)

    store = pltpu.make_async_copy(totals, out, moves.at[1])
    store.start()
    store.wait()


def settle(rows, parts, shape, totals=None):
    fresh = totals is None
    arrays = [array for array, _ in parts]
    entries, place = [], 0
    for index, (array, given) in enumerate(parts):
        for sub, (row, first, fast) in enumerate(given):
            width = array.shape[-3]
            entries.append((index, sub if array.ndim == 4 else None, row, first, width, place, fast))
            place += width
    count = len(arrays)
    given = [] if fresh else [totals]
    return pl.pallas_call(
        functools.partial(settle_kernel, entries=tuple(entries), count=count, fresh=fresh),
        in_specs=[pl.BlockSpec(memory_space=pltpu.SMEM)]
        + [pl.BlockSpec(memory_space=pl.ANY) for _ in arrays]
        + [pl.BlockSpec(memory_space=pl.ANY) for _ in given],
        out_specs=pl.BlockSpec(memory_space=pl.ANY),
        out_shape=jax.ShapeDtypeStruct(shape, jnp.float32),
        scratch_shapes=[
            pltpu.VMEM(shape, jnp.float32),
            pltpu.VMEM((place, *arrays[0].shape[-2:]), jnp.float32),
            pltpu.SemaphoreType.DMA((place,)),
            pltpu.SemaphoreType.DMA((2,)),
        ],
        input_output_aliases={} if fresh else {1 + count: 0},
        name="settle",
    )(rows, *arrays, *given)


def spread(held, axis, paired=False):
    size = lax.axis_size(axis)
    held = held[None]
    span = 1
    while span < size:
        pairs = [(d, d ^ span if paired else (d + span) % size) for d in range(size)]
        got = lax.ppermute(held, axis, pairs)
        held = jnp.concatenate([held, got], axis=0)
        span *= 2
    return held


def place_of(axis, other, paired=False):
    own = lax.axis_index(axis)
    return own ^ other if paired else (own - other) % lax.axis_size(axis)


def partners(reach):
    group = reach + 1
    period = 2 * group
    inner = [[(p ^ x) - p for x in range(1, group)] for p in range(period)]
    options = []
    for picked in itertools.permutations(range(group, period)):
        shifts = [next((v for v in (b - a, b - a - period) if abs(v) <= reach), None) for a, b in enumerate(picked)]
        if None not in shifts:
            options.append((abs(sum(1 if v > 0 else -1 for v in shifts)), shifts))
    options.sort(key=lambda option: option[0])
    for found in itertools.combinations([shifts for _, shifts in options], reach):
        if all(len({shifts[a] for shifts in found}) == reach for a in range(group)):
            break
    outer = [[0] * reach for _ in range(period)]
    for index, shifts in enumerate(found):
        for a, v in enumerate(shifts):
            outer[a][index] = v
            outer[(a + v) % period][index] = -v
    return [a + b for a, b in zip(inner, outer)]


def on_device(tile_flux, tile_frac, weights, block_row, block_col, send_counts):
    steps, kinds = tile_flux.shape[0], tile_flux.shape[1]
    _, num_off, slots, block_rows, _ = weights.shape
    ranks, line = lax.axis_size("gx"), lax.axis_size("gy")
    rank, here = lax.axis_index("gx"), lax.axis_index("gy")
    count = ranks * line
    half = slots // 2
    piece = -(-half // ranks)
    reach = num_off // 2
    shape = (kinds, AB_DEV, 2 * steps, block_rows // 2)
    shifts = partners(reach)
    period = len(shifts)
    near = tuple(range(reach))
    far = tuple(range(reach, 2 * reach))
    shift_here = jnp.array([row + [0] for row in shifts], jnp.int32)[here % period]
    offs = shift_here + reach
    tables = (offs, block_col.transpose(1, 0, 2), send_counts)

    def exchange(value, entry):
        return lax.ppermute(value, AXES, [(d, (d + shifts[d % period][entry]) % count) for d in range(count)])

    def across(value, step, back=False):
        pairs = [(r, (r + step) % ranks) for r in range(ranks)]
        return lax.ppermute(value, "gx", [(b, a) for a, b in pairs] if back else pairs)

    codes = jnp.where(jnp.arange(slots)[None, :] < send_counts[0][:, None], block_row[0], -1)
    family = spread(codes, "gx")
    numbers = jnp.sum(family[:ranks] >= 0, axis=2, dtype=jnp.int32)
    outside = jnp.any(jnp.arange(num_off)[:, None] == offs[None, reach : 2 * reach], axis=1)
    crowded = jnp.any((jnp.sum(numbers > half, axis=0) > 1) & outside)
    family = jnp.where(crowded & (family >= 0), family + AB_DEV, family)

    land, *given = first_products(tables, tile_flux, tile_frac, weights, far, ranks, piece)
    outer, parts = given[: len(far)], given[len(far) :]
    middle = near[1:2]
    inner = {}
    for those in (middle, tuple(e for e in near if e not in middle)):
        inner.update(zip(those, products(tables, land, weights, tuple((e, 0) for e in those), slots)))

    got = {e: exchange(outer[e - reach], e) for e in far}
    lent = [parts[0]] + [across(parts[k], k) for k in range(1, ranks)]
    got.update({e: exchange(inner[e], e) for e in near})
    relay = choose(offs, numbers, lent, far, half)
    passed = [exchange(r, e) for r, e in zip(relay, far)]
    paired = line & (line - 1) == 0
    held = spread(family, "gy", paired)

    sender = (rank * line + here + shift_here) % count
    back_offs = num_off - 1 - offs
    rows = held[place_of("gy", sender % line, paired), place_of("gx", sender // line), back_offs]
    flag = jnp.any(held >= AB_DEV).astype(jnp.int32)
    lives = jnp.sum(rows >= 0, axis=1, keepdims=True, dtype=jnp.int32)
    rows = jnp.concatenate([lives, rows % AB_DEV], axis=1)
    rows = jnp.concatenate([rows, jnp.broadcast_to(flag, (1, rows.shape[1]))], axis=0)

    (mine,) = products(tables, land, weights, ((2 * reach, 0),), slots)
    totals = settle(rows, [(mine, [(2 * reach, 0, False)])], shape)

    def slow(totals):
        more = products(tables, land, weights, tuple((e, half) for e in far), half)
        sent = [exchange(m, e) for m, e in zip(more, far)]
        return settle(rows, [(m, [(e, half, False)]) for m, e in zip(sent, far)], shape, totals)

    totals = lax.cond(flag > 0, slow, lambda totals: totals, totals)
    packed = pack(passed)
    returned = [across(packed, k, back=True) for k in range(1, ranks)]

    early = (near[0], near[1], far[0], far[1])
    totals = settle(rows, [(got[e], [(e, 0, False)]) for e in early], shape, totals)
    parts = [(got[e], [(e, 0, False)]) for e in (*near[2:], *far[2:])]
    parts += [(p, [(e, half, True)]) for p, e in zip(passed, far)]
    parts += [(r, [(e, half + k * piece, True) for e in far]) for k, r in enumerate(returned, 1)]
    totals = settle(rows, parts, shape, totals)
    totals = totals.reshape(kinds, AB_DEV, 2, steps, block_rows // 2).transpose(3, 0, 1, 2, 4)
    return totals.reshape(steps, kinds, AB_DEV * block_rows)


def solution(mesh):
    return jax.shard_map(
        on_device,
        mesh=mesh,
        in_specs=(
            P(None, None, None, AXES),
            P(None, AXES),
            P(AXES, None, None, None, None),
            P(AXES, None, None),
            P(AXES, None, None),
            P(AXES, None),
        ),
        out_specs=P(None, None, AXES),
        check_vma=False,
    )
```

```python
import functools
import itertools

import jax
import jax.numpy as jnp
import numpy as np
from jax import lax
from jax.experimental import pallas as pl
from jax.experimental.pallas import tpu as pltpu
from jax.sharding import PartitionSpec as P


AXES = ("gx", "gy")
AB_DEV = 48
LANES = 128
SUBLANES = 8


def fold_rows(parts):
    row = lax.broadcasted_iota(jnp.int32, parts[0].shape, 0)
    step = SUBLANES // 2
    while step >= 1:
        low = (row // step) % 2 == 0
        half = len(parts) // 2
        merged = []
        for index in range(half):
            first, second = parts[index], parts[index + half]
            keep = jnp.where(low, first, second)
            swap = jnp.where(low, second, first)
            merged.append(keep + jnp.where(low, pltpu.roll(first, SUBLANES - step, 0), pltpu.roll(second, step, 0)))
            del swap
        parts = merged
        step //= 2
    return parts[0]


def merge_blocks(flux_ref, frac_ref, land_ref, first, count):
    steps, kinds = flux_ref.shape[0], flux_ref.shape[1]
    rows = steps * kinds

    @pl.loop(0, count, unroll=2)
    def _(index):
        lanes = pl.ds(pl.multiple_of(index * LANES, LANES), LANES)
        frac = frac_ref[:, pl.ds(pl.multiple_of((first + index) * LANES, LANES), LANES)]
        total = jnp.sum(frac, axis=0, keepdims=True)
        for pair in range(rows // (2 * SUBLANES)):
            pieces = []
            for half in range(2):
                parts = []
                for r in range(SUBLANES):
                    line = (2 * pair + half) * SUBLANES + r
                    parts.append(flux_ref[line % steps, line // steps, :, lanes].astype(jnp.float32) * frac)
                pieces.append(fold_rows(parts) / total)
            value = jnp.concatenate(pieces, axis=0).astype(jnp.bfloat16)
            land_ref[first + index, pl.ds(pair * 2 * SUBLANES, 2 * SUBLANES), :] = value


def block_product(land_ref, col, w_ref, local):
    return lax.dot_general(
        land_ref[col], w_ref[0, 0, local], (((1,), (1,)), ((), ())), preferred_element_type=jnp.float32
    )


def first_kernel(offs_ref, cols_ref, counts_ref, flux, frac, weights, land_out, *refs, far, near, ranks):
    outs, refs = refs[: len(far) + 1 + ranks], refs[len(far) + 1 + ranks :]
    flux_v, frac_v, w_v, land_v, far_v, near_v, piece_v, in_sems, w_sems, out_sems = refs
    groups, half = flux_v.shape[0], w_v.shape[1]
    wide = flux_v.shape[-1]
    piece = piece_v.shape[2]
    blocks = land_v.shape[0] // groups
    chunks = [(e, 0, None) for e in far] + [(near, 0, None), (near, 1, None)] + [(e, 1, i) for i, e in enumerate(far)]

    def load_flux(i):
        return pltpu.make_async_copy(flux.at[:, :, :, pl.ds(i * wide, wide)], flux_v.at[i], in_sems.at[1 + i])

    def load_weights(index):
        entry, part, _ = chunks[index]
        source = weights.at[0, offs_ref[entry], pl.ds(part * half, half)]
        return pltpu.make_async_copy(source, w_v.at[index], w_sems.at[index])

    def used(index):
        entry, part, _ = chunks[index]
        return counts_ref[0, offs_ref[entry]] > part * half

    load_frac = pltpu.make_async_copy(frac, frac_v, in_sems.at[0])
    load_frac.start()
    for i in range(groups):
        load_flux(i).start()
    for index in range(len(chunks)):

        @pl.when(used(index))
        def _():
            load_weights(index).start()

    load_frac.wait()
    for i in range(groups):
        load_flux(i).wait()
        merge_blocks(flux_v.at[i], frac_v, land_v, i * blocks, blocks)
    stores = []

    def store(source, to):
        stores.append(pltpu.make_async_copy(source, to, out_sems.at[len(stores)]))
        stores[-1].start()

    store(land_v, land_out)
    for index, (entry, part, at) in enumerate(chunks):

        @pl.when(used(index))
        def _():
            load_weights(index).wait()
            for local in range(half):
                value = lax.dot_general(
                    land_v[cols_ref[offs_ref[entry], 0, part * half + local]],
                    w_v[index, local],
                    (((1,), (1,)), ((), ())),
                    preferred_element_type=jnp.float32,
                )
                if at is not None:
                    piece_v[local // piece, at, local % piece] = value
                elif entry == near:
                    near_v[part * half + local] = value
                else:
                    far_v[index, local] = value

        if index < len(far):
            store(far_v.at[index], outs[index])
        elif index == len(far) + 1:
            store(near_v, outs[len(far)])
    for k in range(ranks):
        store(piece_v.at[k], outs[len(far) + 1 + k])
    for copy in stores:
        copy.wait()


def first_products(tables, tile_flux, tile_frac, weights, far, near, ranks, piece):
    steps, kinds, tiles, cells = tile_flux.shape
    _, _, slots, rows, cols = weights.shape
    nf, blocks, half = steps * kinds, cells // cols, slots // 2
    groups = min(g for g in range(1, blocks + 1) if blocks % g == 0 and blocks // g <= 4)
    anywhere = pl.BlockSpec(memory_space=pl.ANY)
    shapes = [(half, nf, rows)] * len(far) + [(slots, nf, rows)] + [(len(far), piece, nf, rows)] * ranks
    chunks = 2 * len(far) + 2
    return pl.pallas_call(
        functools.partial(first_kernel, far=far, near=near, ranks=ranks),
        in_specs=[pl.BlockSpec(memory_space=pltpu.SMEM)] * 3 + [anywhere] * 3,
        out_specs=[anywhere] * (1 + len(shapes)),
        out_shape=[jax.ShapeDtypeStruct((blocks, nf, cols), jnp.bfloat16)]
        + [jax.ShapeDtypeStruct(shape, jnp.float32) for shape in shapes],
        scratch_shapes=[
            pltpu.VMEM((groups, steps, kinds, tiles, cells // groups), tile_flux.dtype),
            pltpu.VMEM(tile_frac.shape, tile_frac.dtype),
            pltpu.VMEM((chunks, half, rows, cols), weights.dtype),
            pltpu.VMEM((blocks, nf, cols), jnp.bfloat16),
            pltpu.VMEM((len(far), half, nf, rows), jnp.float32),
            pltpu.VMEM((slots, nf, rows), jnp.float32),
            pltpu.VMEM((ranks, len(far), piece, nf, rows), jnp.float32),
            pltpu.SemaphoreType.DMA((1 + groups,)),
            pltpu.SemaphoreType.DMA((chunks,)),
            pltpu.SemaphoreType.DMA((1 + len(shapes),)),
        ],
        name="first",
    )(*tables, tile_flux, tile_frac, weights)


def product_kernel(offs_ref, cols_ref, counts_ref, land_ref, *refs, chunks):
    for index, (entry, first) in enumerate(chunks):
        w_ref = refs[index]
        out_ref = refs[len(chunks) + index]
        offset = offs_ref[entry]
        for start in range(0, out_ref.shape[0], SUBLANES):

            @pl.when(first + start < counts_ref[0, offset])
            def _():
                for local in range(start, min(start + SUBLANES, out_ref.shape[0])):
                    out_ref[local] = block_product(land_ref, cols_ref[offset, 0, first + local], w_ref, local)


def products(tables, land, weights, chunks, width):
    _, _, _, rows, cols = weights.shape
    blocks, nf, _ = land.shape
    return pl.pallas_call(
        functools.partial(product_kernel, chunks=chunks),
        grid_spec=pltpu.PrefetchScalarGridSpec(
            num_scalar_prefetch=3,
            grid=(1,),
            in_specs=[pl.BlockSpec((blocks, nf, cols), lambda i, *_: (0, 0, 0))]
            + [
                pl.BlockSpec((1, 1, width, rows, cols), lambda i, offs, *_, e=e, f=f: (0, offs[e], f // width, 0, 0))
                for e, f in chunks
            ],
            out_specs=[pl.BlockSpec((width, nf, rows), lambda i, *_: (0, 0, 0)) for _ in chunks],
        ),
        out_shape=[jax.ShapeDtypeStruct((width, nf, rows), jnp.float32) for _ in chunks],
        name="products",
    )(*tables, land, *([weights] * len(chunks)))


def choose_kernel(offs_ref, info_ref, *refs, entries, half, places, at):
    ranks = len(refs) - 1 - len(entries)
    outs, sems = refs[ranks:-1], refs[-1]
    for go in (True, False):
        for index, entry in enumerate(entries):
            pick = jnp.int32(0)
            for rank in reversed(range(ranks)):
                pick = jnp.where(info_ref[places[rank], at + offs_ref[entry]] > half, rank, pick)
            for rank in range(ranks):

                @pl.when(pick == rank)
                def _():
                    copy = pltpu.make_async_copy(refs[rank].at[index], outs[index], sems.at[index])
                    copy.start() if go else copy.wait()


def choose(offs, info, givens, entries, half, places, at):
    return pl.pallas_call(
        functools.partial(choose_kernel, entries=entries, half=half, places=places, at=at),
        in_specs=[pl.BlockSpec(memory_space=pltpu.SMEM)] * 2 + [pl.BlockSpec(memory_space=pl.ANY)] * len(givens),
        out_specs=[pl.BlockSpec(memory_space=pltpu.VMEM)] * len(entries),
        out_shape=[jax.ShapeDtypeStruct(givens[0].shape[1:], jnp.float32)] * len(entries),
        scratch_shapes=[pltpu.SemaphoreType.DMA((len(entries),))],
        name="choose",
    )(offs, info, *givens)


def pack_kernel(*refs):
    givens, out, sems = refs[:-2], refs[-2], refs[-1]
    copies = [pltpu.make_async_copy(g, out.at[i], sems.at[i]) for i, g in enumerate(givens)]
    for copy in copies:
        copy.start()
    for copy in copies:
        copy.wait()


def pack(givens):
    return pl.pallas_call(
        pack_kernel,
        in_specs=[pl.BlockSpec(memory_space=pl.ANY)] * len(givens),
        out_specs=pl.BlockSpec(memory_space=pltpu.VMEM),
        out_shape=jax.ShapeDtypeStruct((len(givens), *givens[0].shape), jnp.float32),
        scratch_shapes=[pltpu.SemaphoreType.DMA((len(givens),))],
        name="pack",
    )(*givens)


def add_block(totals, block, value):
    kinds = totals.shape[0]
    steps = totals.shape[2] // 2
    low = lax.broadcasted_iota(jnp.int32, (2 * steps, LANES), 0) < steps
    for pair in range(kinds // 2):
        lines = pl.ds(pair * 2 * steps, 2 * steps)
        left, right = value[lines, pl.ds(0, LANES)], value[lines, pl.ds(LANES, LANES)]
        totals[2 * pair, block] += jnp.where(low, left, pltpu.roll(right, steps, 0))
        totals[2 * pair + 1, block] += jnp.where(low, pltpu.roll(left, steps, 0), right)


def own_kernel(cols_ref, rows_ref, counts_ref, land_ref, w_ref, totals, made, *, offset):
    totals[...] = jnp.zeros(totals.shape, totals.dtype)
    slots = made.shape[0]
    for start in range(0, slots, SUBLANES):

        @pl.when(start < counts_ref[0, offset])
        def _():
            for local in range(start, min(start + SUBLANES, slots)):
                made[local] = block_product(land_ref, cols_ref[offset, 0, local], w_ref, local)

    @pl.loop(0, counts_ref[0, offset])
    def _(slot):
        add_block(totals, rows_ref[offset, 0, slot], made.at[slot])


def own_totals(block_col, block_row, counts, land, weights, offset, shape):
    _, _, slots, rows, cols = weights.shape
    smem = pl.BlockSpec(memory_space=pltpu.SMEM)
    return pl.pallas_call(
        functools.partial(own_kernel, offset=offset),
        grid=(1,),
        in_specs=[smem] * 3
        + [
            pl.BlockSpec(land.shape, lambda i: (0, 0, 0)),
            pl.BlockSpec((1, 1, slots, rows, cols), lambda i: (0, offset, 0, 0, 0)),
        ],
        out_specs=pl.BlockSpec(shape, lambda i: (0, 0, 0, 0)),
        out_shape=jax.ShapeDtypeStruct(shape, jnp.float32),
        scratch_shapes=[pltpu.VMEM((slots, land.shape[1], rows), jnp.float32)],
        name="own",
    )(block_col, block_row, counts, land, weights)


def settle_kernel(where_ref, flag_ref, info_ref, *refs, entries, count, fresh, slots, at):
    rest = refs[count:]
    given = None if fresh else rest[0]
    out, totals, held, sems, moves = rest[-5:]

    def live(entry):
        _, _, row, first, limit, _, fast = entries[entry]
        number = jnp.clip(info_ref[where_ref[0, row], at + where_ref[1, row]] - first, 0, limit)
        return jnp.where(flag_ref[0] > 0, 0, number) if fast else number

    def copy(entry, slot):
        index, sub, place = entries[entry][0], entries[entry][1], entries[entry][5]
        source = refs[index].at[slot] if sub is None else refs[index].at[sub, slot]
        return pltpu.make_async_copy(source, held.at[place + slot], sems.at[place + slot])

    for entry in range(len(entries)):

        @pl.loop(0, live(entry))
        def _(slot, entry=entry):
            copy(entry, slot).start()

    if fresh:
        totals[...] = jnp.zeros(totals.shape, totals.dtype)
    else:
        load = pltpu.make_async_copy(given, totals, moves.at[0])
        load.start()
        load.wait()
    for entry in range(len(entries)):

        @pl.loop(0, live(entry))
        def _(slot, entry=entry):
            copy(entry, slot).wait()
            _, _, row, first, _, start, _ = entries[entry]
            block = info_ref[where_ref[0, row], where_ref[1, row] * slots + first + slot]
            add_block(totals, block, held.at[start + slot])

    store = pltpu.make_async_copy(totals, out, moves.at[1])
    store.start()
    store.wait()


def settle(tables, parts, shape, slots, at, totals=None):
    fresh = totals is None
    arrays = [array for array, _ in parts]
    entries, place = [], 0
    for index, (array, given) in enumerate(parts):
        for sub, (row, first, fast) in enumerate(given):
            width = array.shape[-3]
            entries.append((index, sub if array.ndim == 4 else None, row, first, width, place, fast))
            place += width
    count = len(arrays)
    given = [] if fresh else [totals]
    return pl.pallas_call(
        functools.partial(
            settle_kernel, entries=tuple(entries), count=count, fresh=fresh, slots=slots, at=at
        ),
        in_specs=[pl.BlockSpec(memory_space=pltpu.SMEM)] * 3
        + [pl.BlockSpec(memory_space=pl.ANY) for _ in arrays]
        + [pl.BlockSpec(memory_space=pl.ANY) for _ in given],
        out_specs=pl.BlockSpec(memory_space=pl.ANY),
        out_shape=jax.ShapeDtypeStruct(shape, jnp.float32),
        scratch_shapes=[
            pltpu.VMEM(shape, jnp.float32),
            pltpu.VMEM((place, *arrays[0].shape[-2:]), jnp.float32),
            pltpu.SemaphoreType.DMA((place,)),
            pltpu.SemaphoreType.DMA((2,)),
        ],
        input_output_aliases={} if fresh else {3 + count: 0},
        name="settle",
    )(*tables, *arrays, *given)


def spans(axis, size):
    return [(axis, 1 << bit) for bit in range((size - 1).bit_length())]


def rounds_of(ranks, line):
    gx, gy = spans("gx", ranks), spans("gy", line)
    return gy[:-1] + gx + gy[-1:]


def spread(held, rounds, *ready):
    known = []
    for axis, span in rounds:
        size = lax.axis_size(axis)
        paired = axis == "gy" and size & (size - 1) == 0
        pairs = [(d, d ^ span if paired else (d + span) % size) for d in range(size)]
        got = lax.ppermute(held, axis, pairs)
        got = lax.optimization_barrier((got, *ready))[0]
        held = jnp.concatenate([held, got], axis=0)
        known.append(held)
    return known


def place_of(rounds, back, along):
    return sum((((back if axis == "gx" else along) & span) != 0) * (1 << bit) for bit, (axis, span) in enumerate(rounds))


def partners(reach):
    group = reach + 1
    period = 2 * group
    inner = [[(p ^ x) - p for x in range(1, group)] for p in range(period)]
    options = []
    for picked in itertools.permutations(range(group, period)):
        shifts = [next((v for v in (b - a, b - a - period) if abs(v) <= reach), None) for a, b in enumerate(picked)]
        if None not in shifts:
            options.append((abs(sum(1 if v > 0 else -1 for v in shifts)), shifts))
    options.sort(key=lambda option: option[0])
    for found in itertools.combinations([shifts for _, shifts in options], reach):
        if all(len({shifts[a] for shifts in found}) == reach for a in range(group)):
            break
    outer = [[0] * reach for _ in range(period)]
    for index, shifts in enumerate(found):
        for a, v in enumerate(shifts):
            outer[a][index] = v
            outer[(a + v) % period][index] = -v
    return [a + b for a, b in zip(inner, outer)]


def on_device(tile_flux, tile_frac, weights, block_row, block_col, send_counts):
    steps, kinds = tile_flux.shape[0], tile_flux.shape[1]
    _, num_off, slots, block_rows, _ = weights.shape
    ranks, line = lax.axis_size("gx"), lax.axis_size("gy")
    rank, here = lax.axis_index("gx"), lax.axis_index("gy")
    count = ranks * line
    half = slots // 2
    piece = -(-half // ranks)
    reach = num_off // 2
    shape = (kinds, AB_DEV, 2 * steps, block_rows // 2)
    shifts = partners(reach)
    period = len(shifts)
    near = tuple(range(reach))
    far = tuple(range(reach, 2 * reach))
    shift_here = jnp.array([row + [0] for row in shifts], jnp.int32)[here % period]
    offs = shift_here + reach
    tables = (offs, block_col.transpose(1, 0, 2), send_counts)

    def exchange(value, entry):
        return lax.ppermute(value, AXES, [(d, (d + shifts[d % period][entry]) % count) for d in range(count)])

    def across(value, step, back=False):
        pairs = [(r, (r + step) % ranks) for r in range(ranks)]
        return lax.ppermute(value, "gx", [(b, a) for a, b in pairs] if back else pairs)

    at = num_off * slots
    info = jnp.concatenate([block_row.reshape(1, at), send_counts], axis=1)
    rounds = rounds_of(ranks, line)
    family = spread(info, rounds[:-1])[-1]
    places = tuple(place_of(rounds, k, 0) for k in range(ranks))

    land, *given = first_products(tables, tile_flux, tile_frac, weights, far, near[1], ranks, piece)
    outer, parts = given[: len(far)], given[len(far) + 1 :]
    those = tuple(e for e in near if e != near[1])
    inner = dict(zip(those, products(tables, land, weights, tuple((e, 0) for e in those), slots)))
    inner[near[1]] = given[len(far)]

    got = {e: exchange(outer[e - reach], e) for e in far}
    lent = [parts[0]] + [across(parts[k], k) for k in range(1, ranks)]
    got.update({e: exchange(inner[e], e) for e in near})
    relay = choose(offs, family, lent, far, half, places, at)
    passed = [exchange(r, e) for r, e in zip(relay, far)]
    packed = pack(passed)
    returned = [across(packed, k, back=True) for k in range(1, ranks)]

    (held,) = spread(family, rounds[-1:], packed)

    sender = (rank * line + here + shift_here) % count
    back_offs = num_off - 1 - offs
    paired = line & (line - 1) == 0

    def along(place):
        return here ^ place if paired else (here - place) % line

    where = jnp.stack([place_of(rounds, (rank - sender // line) % ranks, along(sender % line)), back_offs])
    pick = np.zeros((line, held.shape[0]), np.float32)
    for y in range(line):
        pick[y, [place_of(rounds, k, y) for k in range(ranks)]] = 1
    outside = [[v in row[reach:] for v in range(-reach, reach + 1)] for row in shifts]
    spots = [[outside[(p ^ y if paired else p - y) % period] for y in range(line)] for p in range(period)]
    many = jnp.dot(pick, (held[:, at:] > half).astype(jnp.float32))
    flag = jnp.any((many > 1.5) & jnp.array(spots)[here % period]).astype(jnp.int32).reshape(1)
    settled = (where, flag, held)

    totals = own_totals(tables[1], block_row.transpose(1, 0, 2), send_counts, land, weights, reach, shape)

    def slow(totals):
        more = products(tables, land, weights, tuple((e, half) for e in far), half)
        sent = [exchange(m, e) for m, e in zip(more, far)]
        return settle(settled, [(m, [(e, half, False)]) for m, e in zip(sent, far)], shape, slots, at, totals)

    totals = lax.cond(flag[0] > 0, slow, lambda totals: totals, totals)
    early = (near[0], near[1], far[0], far[1])
    totals = settle(settled, [(got[e], [(e, 0, False)]) for e in early], shape, slots, at, totals)
    parts = [(got[e], [(e, 0, False)]) for e in (*near[2:], *far[2:])]
    parts += [(p, [(e, half, True)]) for p, e in zip(passed, far)]
    parts += [(r, [(e, half + k * piece, True) for e in far]) for k, r in enumerate(returned, 1)]
    totals = settle(settled, parts, shape, slots, at, totals)
    totals = totals.reshape(kinds, AB_DEV, 2, steps, block_rows // 2).transpose(3, 0, 1, 2, 4)
    return totals.reshape(steps, kinds, AB_DEV * block_rows)


def solution(mesh):
    return jax.shard_map(
        on_device,
        mesh=mesh,
        in_specs=(
            P(None, None, None, AXES),
            P(None, AXES),
            P(AXES, None, None, None, None),
            P(AXES, None, None),
            P(AXES, None, None),
            P(AXES, None),
        ),
        out_specs=P(None, None, AXES),
        check_vma=False,
    )
```
